32 devices in a mesh: ctx: 16 (over z, x, core), dp: 2 (over y).
Axes of the slice: x: 2, y: 2, z: 4, core: 2. Of those that a mesh axis runs over, the one named last changes fastest.
Arguments:
- queries: bfloat16 [4096, 1024], P(('dp', 'ctx')), parts along dimension 0, may hold values from -2.5 to 2.5
- keys: bfloat16 [4096, 128], P(('dp', 'ctx')), parts along dimension 0, may hold values from -2.5 to 2.5
- values: bfloat16 [4096, 128], P(('dp', 'ctx')), parts along dimension 0, may hold values from -6 to 6
- grad_out: bfloat16 [4096, 1024], P(('dp', 'ctx')), parts along dimension 0, may hold values from -6 to 6
- pair_order: int32 [32], P('dp'), parts along dimension 0, may hold values from 0 to 15, each once
- doc_lengths: int32 [32], P('dp'), parts along dimension 0, may hold values from 1 to 512, 2048 in all
Outputs:
- attn_out: bfloat16 [4096, 1024], P(('dp', 'ctx')), parts along dimension 0
- query_grad: bfloat16 [4096, 1024], P(('dp', 'ctx')), parts along dimension 0
- key_grad: bfloat16 [4096, 128], P(('dp', 'ctx')), parts along dimension 0
- value_grad: bfloat16 [4096, 128], P(('dp', 'ctx')), parts along dimension 0
The draws below stay inside these ranges and needn't reach their ends.
There are 2 independent parts, one for each index of `dp`. The reference program is written for one: setup_inputs(seed, part) draws one part's arguments, and reference() takes and returns one part's arrays. A program takes and returns all parts, laid end to end along the dimension named above; each array names one. Nothing has to cross between parts.
Inputs may be any that keep to these rules, and one draw needn't show every extreme that they name: A permutation; the device of index d along ctx holds the sequence blocks pair_order[d] and 31 - pair_order[d], of 64 tokens each, in this order. `doc_lengths`: the documents lie end to end in sequence order; the lengths sum to 2048 and the longest has exactly 512 tokens.
All inputs are finite; a program needn't handle non-finite values.
Results may differ from the reference program's by a relative error of at most 0.01.
Values may be sent and summed in bfloat16 or wider, within the bound.
A program may use at most 128 MiB of HBM per device.

```python
import math
import jax
import jax.numpy as jnp
import numpy as np
from jax import lax

HEADS = 8
HDIM = 128
TOK_DEV = 128
DOCS = 16
HALF_DEV = 64
PAIRS = 16
SEQ = 2048


def draw_keys(key, part):
    first_key, second_key = jax.random.split(key, 2)
    row_scales = jnp.exp(jax.random.uniform(first_key, (SEQ, 1), jnp.float32, jnp.log(0.2), jnp.log(2.0)))
    base = jax.random.normal(second_key, (SEQ, HDIM), jnp.float32)
    return jnp.clip(base * row_scales, -2.5, 2.5).astype(jnp.bfloat16)


def block_scale(own_key, dims, cuts, low, top_value):
    def one(axis_at, parts):
        heights = jax.random.uniform(jax.random.fold_in(jax.random.fold_in(own_key, 6), axis_at), (parts,), jnp.float32, low / len(cuts), top_value / len(cuts))
        return jnp.repeat(jnp.exp(heights), dims[axis_at] // parts).reshape((-1,) + (1,) * (len(dims) - axis_at - 1))

    loudness = one(*cuts[0])
    for cut in cuts[1:]:
        loudness = loudness * one(*cut)
    return loudness


def length_profile(number_of, total, reach, skew):
    portions = [(1 << 20) // math.isqrt(standing ** skew) + 1 for standing in range(2, number_of + 1)]
    rest, holding = total - reach - (number_of - 1), [1] * (number_of - 1)
    while rest > 0:
        candidates = [i for i in range(number_of - 1) if holding[i] < reach]
        whole, remaining = sum([portions[i] for i in candidates]), rest
        for i in candidates:
            extra = min(reach - holding[i], max(1, remaining * portions[i] // whole), rest)
            holding[i] = holding[i] + extra
            rest = rest - extra
    return np.array([reach] + holding)


def uneven(stream_key, number_of, total, limit, skew):
    if number_of == 2:
        one = jax.random.randint(stream_key, (), max(1, total - limit), min(limit, total - 1) + 1)
        return jnp.stack([one, total - one])
    tallies = jnp.asarray(length_profile(number_of, total, limit, skew), jnp.int32)
    couples = (number_of - 1) // 2
    source_of, taker = tallies[1:1 + 2 * couples:2], tallies[2:2 + 2 * couples:2]
    room = jnp.minimum(source_of - 1, limit - taker)
    moved = jax.random.randint(jax.random.fold_in(stream_key, 1), (couples,), 0, 1 << 20) % (room + 1)
    tallies = tallies.at[1:1 + 2 * couples:2].set(source_of - moved).at[2:2 + 2 * couples:2].set(taker + moved)
    return tallies[jax.random.permutation(jax.random.fold_in(stream_key, 2), number_of)]


def centred(rng, extent, spread, most, pieces=(), kind=jnp.bfloat16):
    level = block_scale(rng, extent, pieces, -0.22, 0.18) if pieces else 1.0
    values = jax.random.normal(rng, extent, jnp.float32) * spread * level
    return jnp.minimum(jnp.maximum(values, -most), most).astype(kind)


def setup_inputs(seed: int = 0, part: int = 0) -> dict:
    streams_of = jax.random.split(jax.random.key(seed), 7)
    part_splits = jax.random.split(jax.random.fold_in(streams_of[6], part), 7)
    queries = centred(part_splits[0], (SEQ, HEADS * HDIM), 1.0, 2.5, ((0, 16),))
    keys = draw_keys(jax.random.fold_in(jax.random.fold_in(streams_of[6], part), 71), part)
    values = centred(part_splits[2], (SEQ, HDIM), 1.0, 6.0, ((0, 16),))
    grad_out = centred(part_splits[3], (SEQ, HEADS * HDIM), 1.0, 6.0, ((0, 16),))
    pair_order = jax.random.permutation(part_splits[4], PAIRS).astype(jnp.int32)
    doc_lengths = uneven(part_splits[5], DOCS, SEQ, SEQ // 4, 2).astype(jnp.int32)
    return dict(queries=queries, keys=keys, values=values, grad_out=grad_out, pair_order=pair_order, doc_lengths=doc_lengths)


def token_labels(pair_order, doc_lengths):
    row_ids = jnp.arange(SEQ, dtype=jnp.int32)
    shard_ids = row_ids // TOK_DEV
    inside = row_ids % TOK_DEV
    paired = pair_order[shard_ids].astype(jnp.int32)
    seq_block = jnp.where(inside < HALF_DEV, paired, 2 * PAIRS - 1 - paired)
    position = (seq_block * HALF_DEV + inside % HALF_DEV).astype(jnp.int32)
    doc_ends = jnp.cumsum(doc_lengths).astype(jnp.int32)
    document = jnp.sum((doc_ends[None, :] <= position[:, None]).astype(jnp.int32), axis=1)
    return position, document


def reference(queries, keys, values, grad_out, pair_order, doc_lengths):
    position, document = token_labels(pair_order, doc_lengths)
    score_scale = HDIM ** -0.5
    highest = lax.Precision.HIGHEST
    keys_f32 = keys.astype(jnp.float32)
    values_f32 = values.astype(jnp.float32)
    query_block = min(SEQ, 256)
    block_count = SEQ // query_block
    query_parts = queries.reshape(block_count, query_block, HEADS, HDIM)
    grad_parts = grad_out.reshape(block_count, query_block, HEADS, HDIM)
    pos_parts = position.reshape(block_count, query_block)
    doc_parts = document.reshape(block_count, query_block)

    def one_block(carried, sliced):
        key_acc, value_acc = carried
        query_rows, grad_rows, query_pos, query_doc = sliced
        query_f32 = query_rows.astype(jnp.float32)
        grad_f32 = grad_rows.astype(jnp.float32)
        allowed = (query_doc[:, None] == document[None, :]) & (position[None, :] <= query_pos[:, None])
        scores = jnp.einsum("thd,kd->thk", query_f32, keys_f32, precision=highest) * score_scale
        exp_scores = jnp.where(allowed[:, None, :], jnp.exp(scores), jnp.float32(0.0))
        totals = jnp.sum(exp_scores, axis=2)
        weight_b = lax.optimization_barrier(exp_scores.astype(jnp.bfloat16)).astype(jnp.float32)
        attn_out = (jnp.einsum("thk,kd->thd", weight_b, values_f32, precision=highest) / totals[:, :, None]).astype(jnp.bfloat16)
        log_totals = jnp.log(totals)
        row_dots = jnp.sum(grad_f32 * attn_out.astype(jnp.float32), axis=2)
        prob_f32 = jnp.where(allowed[:, None, :], jnp.exp(scores - log_totals[:, :, None]), jnp.float32(0.0))
        prob_b = lax.optimization_barrier(prob_f32.astype(jnp.bfloat16)).astype(jnp.float32)
        grad_prob = jnp.einsum("thd,kd->thk", grad_f32, values_f32, precision=highest)
        grad_score = lax.optimization_barrier((prob_f32 * (grad_prob - row_dots[:, :, None])).astype(jnp.bfloat16)).astype(jnp.float32)
        query_grad = (score_scale * jnp.einsum("thk,kd->thd", grad_score, keys_f32, precision=highest)).astype(jnp.bfloat16)
        key_acc = key_acc + jnp.einsum("thk,thd->kd", grad_score, query_f32, precision=highest)
        value_acc = value_acc + jnp.einsum("thk,thd->kd", prob_b, grad_f32, precision=highest)
        return (key_acc, value_acc), (attn_out, query_grad)

    start_sums = (jnp.zeros((SEQ, HDIM), jnp.float32), jnp.zeros((SEQ, HDIM), jnp.float32))
    final_sums, stacked = lax.scan(one_block, start_sums, (query_parts, grad_parts, pos_parts, doc_parts))
    attn_out = stacked[0].reshape(SEQ, HEADS * HDIM)
    query_grad = stacked[1].reshape(SEQ, HEADS * HDIM)
    key_grad = (score_scale * final_sums[0]).astype(jnp.bfloat16)
    value_grad = final_sums[1].astype(jnp.bfloat16)
    return (attn_out, query_grad, key_grad, value_grad)
```

```python
import functools

import jax
import jax.numpy as jnp
from jax import lax
from jax.experimental import pallas as pl
from jax.experimental.pallas import tpu as pltpu
from jax.sharding import PartitionSpec as P

MESH = pl.DeviceIdType.MESH
VMEM_LIMIT = 64 * 1024 * 1024 - 128 * 1024


def flip(index, mask):
    bit = 1
    while bit <= mask:
        if mask & bit:
            index = index + bit - 2 * bit * (lax.div(index, bit) % 2)
        bit *= 2
    return index


def place(n):
    me = lax.axis_index("ctx")
    core = me % 2
    x = lax.div(me, 2) % 2
    z = lax.div(me, 4)
    return z, x, core


def index_of(z, x, core):
    return (z * 2 + x) * 2 + core


def z_order(depth):
    return sorted(range(1, depth), key=lambda mask: (-(mask & -mask), mask))


def greet(depth, z, x, core):
    barrier = pltpu.get_barrier_semaphore()
    peers = [index_of(flip(z, mask), x, core) for mask in z_order(depth)]
    peers += [index_of(z, 1 - x, core), index_of(z, x, 1 - core)]
    for peer in peers:
        pl.semaphore_signal(
            barrier, inc=1, device_id={"ctx": peer}, device_id_type=MESH
        )
    pl.semaphore_wait(barrier, len(peers))


def gather_kernel(n, k_ref, v_ref, all_ref, local_sem, zs, zr, xs, xr, cs, cr):
    depth = n // 4
    z, x, core = place(n)
    me = index_of(z, x, core)
    greet(depth, z, x, core)
    x_peer = index_of(z, 1 - x, core)
    c_peer = index_of(z, x, 1 - core)
    order = z_order(depth)
    sent = []

    def send(src, dst, send_sem, recv_sem, peer):
        copy = pltpu.make_async_remote_copy(
            src_ref=src, dst_ref=dst, send_sem=send_sem, recv_sem=recv_sem,
            device_id={"ctx": peer}, device_id_type=MESH,
        )
        copy.start()
        return copy

    def send_own(send_sem, recv_sem, peer):
        for part, ref in enumerate((k_ref, v_ref)):
            send(ref, all_ref.at[me, part], send_sem, recv_sem, peer)
        sent.append((all_ref.at[me], send_sem))

    def forward(slot, send_sem, recv_sem, peer):
        send(all_ref.at[slot], all_ref.at[slot], send_sem, recv_sem, peer)
        sent.append((all_ref.at[slot], send_sem))

    def wait_for(ref, sem):
        pltpu.make_async_copy(ref, ref, sem).wait()

    for mask in order:
        send_own(zs.at[mask], zr.at[mask], index_of(flip(z, mask), x, core))
    send_own(xs.at[0], xr.at[0], x_peer)
    send_own(cs.at[0, 0], cr.at[0, 0], c_peer)
    local = [
        pltpu.make_async_copy(ref, all_ref.at[me, part], local_sem.at[part])
        for part, ref in enumerate((k_ref, v_ref))
    ]
    for copy in local:
        copy.start()

    arrival = [0] + order[::-1]
    for mask in order[::-1]:
        slot = index_of(flip(z, mask), x, core)
        wait_for(all_ref.at[slot], zr.at[mask])
        forward(slot, xs.at[mask], xr.at[mask], x_peer)
        forward(slot, cs.at[0, mask], cr.at[0, mask], c_peer)
    for mask in arrival:
        slot = index_of(flip(z, mask), 1 - x, core)
        wait_for(all_ref.at[slot], xr.at[mask])
        forward(slot, cs.at[1, mask], cr.at[1, mask], c_peer)
    for mask in arrival:
        for side in range(2):
            slot = index_of(flip(z, mask), 1 - x if side else x, 1 - core)
            wait_for(all_ref.at[slot], cr.at[side, mask])
    for copy in local:
        copy.wait()
    for ref, sem in sent:
        wait_for(ref, sem)


def scatter_kernel(
    n, scale, part_ref, kg_ref, vg_ref, r1, r2, r3, s1, s2, cs, cr, xs, xr, zs, zr
):
    depth = n // 4
    z, x, core = place(n)
    greet(depth, z, x, core)
    head_dim = kg_ref.shape[1]
    x_peer = index_of(z, 1 - x, core)
    c_peer = index_of(z, x, 1 - core)
    order = z_order(depth) + [0]
    sent = []

    def send(src, dst, send_sem, recv_sem, peer):
        copy = pltpu.make_async_remote_copy(
            src_ref=src, dst_ref=dst, send_sem=send_sem, recv_sem=recv_sem,
            device_id={"ctx": peer}, device_id_type=MESH,
        )
        copy.start()
        sent.append(copy)
        return copy

    first, second, third = {}, {}, {}
    for side in (1, 0):
        for mask in order:
            row = flip(z, mask)
            slot = index_of(row, 1 - x if side else x, 1 - core)
            first[side, mask] = send(
                part_ref.at[slot], r1.at[side, mask],
                cs.at[side, mask], cr.at[side, mask], c_peer,
            )
    for mask in order:
        first[1, mask].wait_recv()
        mine = part_ref[index_of(flip(z, mask), 1 - x, core)].astype(jnp.float32)
        s1[mask] = (mine + r1[1, mask].astype(jnp.float32)).astype(jnp.bfloat16)
        second[mask] = send(s1.at[mask], r2.at[mask], xs.at[mask], xr.at[mask], x_peer)
    for mask in order:
        first[0, mask].wait_recv()
        second[mask].wait_recv()
        mine = part_ref[index_of(flip(z, mask), x, core)].astype(jnp.float32)
        mine = mine + r1[0, mask].astype(jnp.float32) + r2[mask].astype(jnp.float32)
        if mask:
            s2[mask] = mine.astype(jnp.bfloat16)
            third[mask] = send(
                s2.at[mask], r3.at[mask], zs.at[mask], zr.at[mask],
                index_of(flip(z, mask), x, core),
            )
        else:
            total = mine
    for mask in order[-2::-1]:
        third[mask].wait_recv()
        total = total + r3[mask].astype(jnp.float32)
    kg_ref[...] = (scale * total[:, :head_dim]).astype(kg_ref.dtype)
    vg_ref[...] = total[:, head_dim:].astype(vg_ref.dtype)
    for copy in sent:
        copy.wait_send()


def attend_kernel(
    n, heads, blocks, pair_ref, doc_ref, q_ref, g_ref, kv_ref,
    o_ref, dq_ref, part_ref, owner, k_buf, v_buf, e_buf, o_acc, dq_acc,
):
    tokens = q_ref.shape[0]
    rows = tokens // 2
    head_dim = q_ref.shape[1] // heads
    wide = heads * rows
    keys = blocks * rows
    scale = head_dim ** (-0.5)
    f32 = jnp.float32

    def put(i, carry):
        owner[pair_ref[i]] = i
        return carry

    lax.fori_loop(0, n, put, 0)
    part_ref[...] = jnp.zeros_like(part_ref)
    pair = pair_ref[lax.axis_index("ctx")]

    def locate(block):
        block = jnp.minimum(block, 2 * n - 1)
        late = block >= n
        dev = owner[jnp.where(late, 2 * n - 1 - block, block)]
        row = pl.multiple_of(jnp.where(late, rows, 0), rows)
        return dev, pl.ds(row, rows)

    def stack(ref, half):
        return jnp.concatenate(
            [
                ref[half * rows:(half + 1) * rows, h * head_dim:(h + 1) * head_dim]
                for h in range(heads)
            ],
            axis=0,
        )

    def unstack(ref, half, flat):
        for h in range(heads):
            ref[half * rows:(half + 1) * rows, h * head_dim:(h + 1) * head_dim] = flat[
                h * rows:(h + 1) * rows
            ].astype(ref.dtype)

    for half in range(2):
        block = 2 * n - 1 - pair if half else pair
        q_pos = block * rows + lax.broadcasted_iota(jnp.int32, (1, wide), 1) % rows

        def starts(i, carry):
            begin, of_rows, of_first = carry
            of_rows = jnp.where(begin <= q_pos, begin, of_rows)
            of_first = jnp.where(begin <= block * rows, begin, of_first)
            return begin + doc_ref[i], of_rows, of_first

        _, q_start, first = lax.fori_loop(
            0, doc_ref.shape[0], starts,
            (jnp.int32(0), jnp.zeros((1, wide), jnp.int32), jnp.int32(0)),
        )
        begin_block = lax.div(first, rows)
        chunks = lax.div(block - begin_block, blocks) + 1
        q_flat = stack(q_ref, half)
        g_flat = stack(g_ref, half)
        o_acc[...] = jnp.zeros_like(o_acc)
        dq_acc[...] = jnp.zeros_like(dq_acc)

        def fetch(chunk):
            for i in range(blocks):
                dev, where = locate(begin_block + chunk * blocks + i)
                k_buf[i * rows:(i + 1) * rows] = kv_ref[dev, 0, where, :]
                v_buf[i * rows:(i + 1) * rows] = kv_ref[dev, 1, where, :]
            return k_buf[...], v_buf[...]

        def forward(chunk, total):
            k, v = fetch(chunk)
            scores = lax.dot_general(
                k, q_flat, (((1,), (1,)), ((), ())), preferred_element_type=f32
            )
            k_pos = (begin_block + chunk * blocks) * rows + lax.broadcasted_iota(
                jnp.int32, (keys, 1), 0
            )
            seen = (k_pos >= q_start) & (k_pos <= q_pos)
            exp_scores = jnp.where(seen, jnp.exp(scores * scale), 0.0)
            e_buf[chunk] = exp_scores
            o_acc[...] += lax.dot_general(
                v, exp_scores.astype(jnp.bfloat16), (((0,), (0,)), ((), ())),
                preferred_element_type=f32,
            )
            return total + jnp.sum(exp_scores, axis=0, keepdims=True)

        total = lax.fori_loop(0, chunks, forward, jnp.zeros((1, wide), f32))
        inverse = 1.0 / total
        out = (o_acc[...] / total).astype(jnp.bfloat16).astype(f32)
        unstack(o_ref, half, out.T)
        row_dot = jnp.sum(g_flat.astype(f32).T * out, axis=0, keepdims=True)

        def backward(chunk, carry):
            k, v = fetch(chunk)
            prob = e_buf[chunk] * inverse
            grad_prob = lax.dot_general(
                v, g_flat, (((1,), (1,)), ((), ())), preferred_element_type=f32
            )
            grad_score = (prob * (grad_prob - row_dot)).astype(jnp.bfloat16)
            dq_acc[...] += lax.dot_general(
                k, grad_score, (((0,), (0,)), ((), ())), preferred_element_type=f32
            )
            dk = jnp.dot(grad_score, q_flat, preferred_element_type=f32)
            dv = jnp.dot(prob.astype(jnp.bfloat16), g_flat, preferred_element_type=f32)
            for i in range(blocks):
                at = begin_block + chunk * blocks + i
                dev, where = locate(at)

                @pl.when(at <= block)
                def _():
                    cut = slice(i * rows, (i + 1) * rows)
                    for side, grad in enumerate((dk, dv)):
                        cols = slice(side * head_dim, (side + 1) * head_dim)
                        old = part_ref[dev, where, cols].astype(f32)
                        part_ref[dev, where, cols] = (old + grad[cut]).astype(jnp.bfloat16)

            return carry

        lax.fori_loop(0, chunks, backward, 0)
        unstack(dq_ref, half, (scale * dq_acc[...]).T)


def shards(queries, keys, values, grad_out, pair_order, doc_lengths):
    tokens, width = queries.shape
    head_dim = keys.shape[1]
    heads = width // head_dim
    n = lax.axis_size("ctx")
    depth = n // 4
    blocks = 4
    vmem = pl.BlockSpec(memory_space=pltpu.VMEM)
    smem = pl.BlockSpec(memory_space=pltpu.SMEM)
    dma = pltpu.SemaphoreType.DMA
    bf16, f32 = jnp.bfloat16, jnp.float32

    gathered = pl.pallas_call(
        functools.partial(gather_kernel, n),
        out_shape=jax.ShapeDtypeStruct((n, 2, tokens, head_dim), bf16),
        in_specs=[vmem] * 2,
        out_specs=vmem,
        scratch_shapes=[
            dma((2,)), dma((depth,)), dma((depth,)), dma((depth,)), dma((depth,)),
            dma((2, depth)), dma((2, depth)),
        ],
        compiler_params=pltpu.CompilerParams(
            collective_id=0, has_side_effects=True, vmem_limit_bytes=VMEM_LIMIT
        ),
        name="gather",
    )(keys, values)

    rows = tokens // 2
    wide = heads * rows
    attn_out, query_grad, terms = pl.pallas_call(
        functools.partial(attend_kernel, n, heads, blocks),
        out_shape=(
            jax.ShapeDtypeStruct((tokens, width), bf16),
            jax.ShapeDtypeStruct((tokens, width), bf16),
            jax.ShapeDtypeStruct((n, tokens, 2 * head_dim), bf16),
        ),
        in_specs=[smem, smem, vmem, vmem, vmem],
        out_specs=(vmem, vmem, vmem),
        scratch_shapes=[
            pltpu.SMEM((n,), jnp.int32),
            pltpu.VMEM((blocks * rows, head_dim), bf16),
            pltpu.VMEM((blocks * rows, head_dim), bf16),
            pltpu.VMEM((2 * n // blocks, blocks * rows, wide), f32),
            pltpu.VMEM((head_dim, wide), f32),
            pltpu.VMEM((head_dim, wide), f32),
        ],
        compiler_params=pltpu.CompilerParams(vmem_limit_bytes=VMEM_LIMIT),
        name="attend",
    )(pair_order, doc_lengths, queries, grad_out, gathered)

    term = (tokens, 2 * head_dim)
    key_grad, value_grad = pl.pallas_call(
        functools.partial(scatter_kernel, n, head_dim ** (-0.5)),
        out_shape=(jax.ShapeDtypeStruct((tokens, head_dim), bf16),) * 2,
        in_specs=[vmem],
        out_specs=(vmem, vmem),
        scratch_shapes=[
            pltpu.VMEM((2, depth) + term, bf16),
            pltpu.VMEM((depth,) + term, bf16),
            pltpu.VMEM((depth,) + term, bf16),
            pltpu.VMEM((depth,) + term, bf16),
            pltpu.VMEM((depth,) + term, bf16),
            dma((2, depth)), dma((2, depth)), dma((depth,)), dma((depth,)),
            dma((depth,)), dma((depth,)),
        ],
        compiler_params=pltpu.CompilerParams(
            collective_id=1, has_side_effects=True, vmem_limit_bytes=VMEM_LIMIT
        ),
        name="scatter",
    )(terms)
    return attn_out, query_grad, key_grad, value_grad


def solution(mesh):
    tokens = P(("dp", "ctx"), None)
    return jax.shard_map(
        shards,
        mesh=mesh,
        in_specs=(tokens, tokens, tokens, tokens, P("dp"), P("dp")),
        out_specs=(tokens,) * 4,
        check_vma=False,
    )
```

```python
import functools

import jax
import jax.numpy as jnp
from jax import lax
from jax.experimental import pallas as pl
from jax.experimental.pallas import tpu as pltpu
from jax.sharding import PartitionSpec as P

MESH = pl.DeviceIdType.MESH
VMEM_LIMIT = 64 * 1024 * 1024 - 128 * 1024


def flip(index, mask):
    bit = 1
    while bit <= mask:
        if mask & bit:
            index = index + bit - 2 * bit * (lax.div(index, bit) % 2)
        bit *= 2
    return index


def place(n):
    me = lax.axis_index("ctx")
    core = me % 2
    x = lax.div(me, 2) % 2
    z = lax.div(me, 4)
    return z, x, core


def index_of(z, x, core):
    return (z * 2 + x) * 2 + core


def z_order(depth):
    return list(range(1, depth))


def greet(depth, z, x, core):
    barrier = pltpu.get_barrier_semaphore()
    peers = [index_of(flip(z, mask), x, core) for mask in z_order(depth)]
    peers += [index_of(z, 1 - x, core), index_of(z, x, 1 - core)]
    for peer in peers:
        pl.semaphore_signal(
            barrier, inc=1, device_id={"ctx": peer}, device_id_type=MESH
        )
    pl.semaphore_wait(barrier, len(peers))


def gather_kernel(n, k_ref, v_ref, all_ref, local_sem, zs, zr, xs, xr, cs, cr):
    depth = n // 4
    z, x, core = place(n)
    me = index_of(z, x, core)
    greet(depth, z, x, core)
    x_peer = index_of(z, 1 - x, core)
    c_peer = index_of(z, x, 1 - core)
    order = z_order(depth)
    sent = []

    def send(src, dst, send_sem, recv_sem, peer):
        copy = pltpu.make_async_remote_copy(
            src_ref=src, dst_ref=dst, send_sem=send_sem, recv_sem=recv_sem,
            device_id={"ctx": peer}, device_id_type=MESH,
        )
        copy.start()
        return copy

    def send_own(send_sem, recv_sem, peer):
        for part, ref in enumerate((k_ref, v_ref)):
            dst = all_ref.at[me, part]
            send(ref, dst, send_sem.at[part], recv_sem.at[part], peer)
            sent.append((dst, send_sem.at[part]))

    def wait_for(ref, sem):
        pltpu.make_async_copy(ref, ref, sem).wait()

    def pass_on(slot, arrived, routes):
        for part in range(2):
            ref = all_ref.at[slot, part]
            wait_for(ref, arrived.at[part])
            for send_sem, recv_sem, peer in routes:
                send(ref, ref, send_sem.at[part], recv_sem.at[part], peer)
                sent.append((ref, send_sem.at[part]))

    send_own(xs.at[0], xr.at[0], x_peer)
    for mask in order:
        send_own(zs.at[mask], zr.at[mask], index_of(flip(z, mask), x, core))
    send_own(cs.at[0, 0], cr.at[0, 0], c_peer)
    local = [
        pltpu.make_async_copy(ref, all_ref.at[me, part], local_sem.at[part])
        for part, ref in enumerate((k_ref, v_ref))
    ]
    for copy in local:
        copy.start()

    def from_z(mask):
        pass_on(
            index_of(flip(z, mask), x, core), zr.at[mask],
            [(xs.at[mask], xr.at[mask], x_peer), (cs.at[0, mask], cr.at[0, mask], c_peer)],
        )

    def from_x(mask):
        pass_on(
            index_of(flip(z, mask), 1 - x, core), xr.at[mask],
            [(cs.at[1, mask], cr.at[1, mask], c_peer)],
        )

    for mask in order:
        from_z(mask)
        if mask == 1:
            from_x(0)
    if depth == 1:
        from_x(0)
    for mask in order:
        from_x(mask)
    for mask in [0] + order:
        for side in range(2):
            slot = index_of(flip(z, mask), 1 - x if side else x, 1 - core)
            pass_on(slot, cr.at[side, mask], [])
    for copy in local:
        copy.wait()
    for ref, sem in sent:
        wait_for(ref, sem)


def scatter_kernel(
    n, scale, part_ref, kg_ref, vg_ref, r1, r2, r3, s1, s2, cs, cr, xs, xr, zs, zr
):
    depth = n // 4
    z, x, core = place(n)
    greet(depth, z, x, core)
    x_peer = index_of(z, 1 - x, core)
    c_peer = index_of(z, x, 1 - core)
    order = z_order(depth)[::-1] + [0]
    sent = []

    def send(src, dst, send_sem, recv_sem, peer):
        copy = pltpu.make_async_remote_copy(
            src_ref=src, dst_ref=dst, send_sem=send_sem, recv_sem=recv_sem,
            device_id={"ctx": peer}, device_id_type=MESH,
        )
        copy.start()
        sent.append(copy)
        return copy

    first, second, third = {}, {}, {}
    for side in (1, 0):
        for mask in order:
            row = flip(z, mask)
            slot = index_of(row, 1 - x if side else x, 1 - core)
            first[side, mask] = send(
                part_ref.at[slot], r1.at[side, mask],
                cs.at[side, mask], cr.at[side, mask], c_peer,
            )
    for mask in order:
        first[1, mask].wait_recv()
        for part in range(2):
            mine = part_ref[index_of(flip(z, mask), 1 - x, core), part].astype(jnp.float32)
            mine = mine + r1[1, mask, part].astype(jnp.float32)
            s1[mask, part] = mine.astype(jnp.bfloat16)
            second[mask, part] = send(
                s1.at[mask, part], r2.at[mask, part],
                xs.at[mask, part], xr.at[mask, part], x_peer,
            )
    total = [None, None]
    for mask in order:
        first[0, mask].wait_recv()
        for part in range(2):
            mine = part_ref[index_of(flip(z, mask), x, core), part].astype(jnp.float32)
            mine = mine + r1[0, mask, part].astype(jnp.float32)
            second[mask, part].wait_recv()
            mine = mine + r2[mask, part].astype(jnp.float32)
            if mask:
                s2[mask, part] = mine.astype(jnp.bfloat16)
                third[mask, part] = send(
                    s2.at[mask, part], r3.at[mask, part],
                    zs.at[mask, part], zr.at[mask, part],
                    index_of(flip(z, mask), x, core),
                )
            else:
                total[part] = mine
    for mask in order[:-1]:
        for part in range(2):
            third[mask, part].wait_recv()
            total[part] = total[part] + r3[mask, part].astype(jnp.float32)
    kg_ref[...] = (scale * total[0]).astype(kg_ref.dtype)
    vg_ref[...] = total[1].astype(vg_ref.dtype)
    for copy in sent:
        copy.wait_send()


def attend_kernel(
    n, heads, blocks, pair_ref, doc_ref, q_ref, g_ref, kv_ref,
    o_ref, dq_ref, part_ref, owner, k_buf, v_buf, e_buf, o_acc, dq_acc,
):
    tokens = q_ref.shape[0]
    rows = tokens // 2
    head_dim = q_ref.shape[1] // heads
    wide = heads * rows
    keys = blocks * rows
    scale = head_dim ** (-0.5)
    f32 = jnp.float32

    def put(i, carry):
        owner[pair_ref[i]] = i
        return carry

    lax.fori_loop(0, n, put, 0)
    part_ref[...] = jnp.zeros_like(part_ref)
    pair = pair_ref[lax.axis_index("ctx")]

    def locate(block):
        block = jnp.minimum(block, 2 * n - 1)
        late = block >= n
        dev = owner[jnp.where(late, 2 * n - 1 - block, block)]
        row = pl.multiple_of(jnp.where(late, rows, 0), rows)
        return dev, pl.ds(row, rows)

    def stack(ref, half):
        return jnp.concatenate(
            [
                ref[half * rows:(half + 1) * rows, h * head_dim:(h + 1) * head_dim]
                for h in range(heads)
            ],
            axis=0,
        )

    def unstack(ref, half, flat):
        for h in range(heads):
            ref[half * rows:(half + 1) * rows, h * head_dim:(h + 1) * head_dim] = flat[
                h * rows:(h + 1) * rows
            ].astype(ref.dtype)

    for half in range(2):
        block = 2 * n - 1 - pair if half else pair
        q_pos = block * rows + lax.broadcasted_iota(jnp.int32, (1, wide), 1) % rows

        def starts(i, carry):
            begin, of_rows, of_first = carry
            of_rows = jnp.where(begin <= q_pos, begin, of_rows)
            of_first = jnp.where(begin <= block * rows, begin, of_first)
            return begin + doc_ref[i], of_rows, of_first

        _, q_start, first = lax.fori_loop(
            0, doc_ref.shape[0], starts,
            (jnp.int32(0), jnp.zeros((1, wide), jnp.int32), jnp.int32(0)),
        )
        begin_block = lax.div(first, rows)
        chunks = lax.div(block - begin_block, blocks) + 1
        q_flat = stack(q_ref, half)
        g_flat = stack(g_ref, half)
        o_acc[...] = jnp.zeros_like(o_acc)
        dq_acc[...] = jnp.zeros_like(dq_acc)

        def fetch(chunk):
            for i in range(blocks):
                dev, where = locate(begin_block + chunk * blocks + i)
                k_buf[i * rows:(i + 1) * rows] = kv_ref[dev, 0, where, :]
                v_buf[i * rows:(i + 1) * rows] = kv_ref[dev, 1, where, :]
            return k_buf[...], v_buf[...]

        def forward(chunk, total):
            k, v = fetch(chunk)
            scores = lax.dot_general(
                k, q_flat, (((1,), (1,)), ((), ())), preferred_element_type=f32
            )
            k_pos = (begin_block + chunk * blocks) * rows + lax.broadcasted_iota(
                jnp.int32, (keys, 1), 0
            )
            seen = (k_pos >= q_start) & (k_pos <= q_pos)
            exp_scores = jnp.where(seen, jnp.exp(scores * scale), 0.0)
            e_buf[chunk] = exp_scores
            o_acc[...] += lax.dot_general(
                v, exp_scores.astype(jnp.bfloat16), (((0,), (0,)), ((), ())),
                preferred_element_type=f32,
            )
            return total + jnp.sum(exp_scores, axis=0, keepdims=True)

        total = lax.fori_loop(0, chunks, forward, jnp.zeros((1, wide), f32))
        inverse = 1.0 / total
        out = (o_acc[...] / total).astype(jnp.bfloat16).astype(f32)
        unstack(o_ref, half, out.T)
        row_dot = jnp.sum(g_flat.astype(f32).T * out, axis=0, keepdims=True)

        def backward(chunk, carry):
            k, v = fetch(chunk)
            prob = e_buf[chunk] * inverse
            grad_prob = lax.dot_general(
                v, g_flat, (((1,), (1,)), ((), ())), preferred_element_type=f32
            )
            grad_score = (prob * (grad_prob - row_dot)).astype(jnp.bfloat16)
            dq_acc[...] += lax.dot_general(
                k, grad_score, (((0,), (0,)), ((), ())), preferred_element_type=f32
            )
            dk = jnp.dot(grad_score, q_flat, preferred_element_type=f32)
            dv = jnp.dot(prob.astype(jnp.bfloat16), g_flat, preferred_element_type=f32)
            for i in range(blocks):
                at = begin_block + chunk * blocks + i
                dev, where = locate(at)

                @pl.when(at <= block)
                def _():
                    cut = slice(i * rows, (i + 1) * rows)
                    for side, grad in enumerate((dk, dv)):
                        old = part_ref[dev, side, where, :].astype(f32)
                        part_ref[dev, side, where, :] = (old + grad[cut]).astype(jnp.bfloat16)

            return carry

        lax.fori_loop(0, chunks, backward, 0)
        unstack(dq_ref, half, (scale * dq_acc[...]).T)


def shards(queries, keys, values, grad_out, pair_order, doc_lengths):
    tokens, width = queries.shape
    head_dim = keys.shape[1]
    heads = width // head_dim
    n = lax.axis_size("ctx")
    depth = n // 4
    blocks = 4
    vmem = pl.BlockSpec(memory_space=pltpu.VMEM)
    smem = pl.BlockSpec(memory_space=pltpu.SMEM)
    dma = pltpu.SemaphoreType.DMA
    bf16, f32 = jnp.bfloat16, jnp.float32

    gathered = pl.pallas_call(
        functools.partial(gather_kernel, n),
        out_shape=jax.ShapeDtypeStruct((n, 2, tokens, head_dim), bf16),
        in_specs=[vmem] * 2,
        out_specs=vmem,
        scratch_shapes=[
            dma((2,)), dma((depth, 2)), dma((depth, 2)), dma((depth, 2)), dma((depth, 2)),
            dma((2, depth, 2)), dma((2, depth, 2)),
        ],
        compiler_params=pltpu.CompilerParams(
            collective_id=0, has_side_effects=True, vmem_limit_bytes=VMEM_LIMIT
        ),
        name="gather",
    )(keys, values)

    rows = tokens // 2
    wide = heads * rows
    attn_out, query_grad, terms = pl.pallas_call(
        functools.partial(attend_kernel, n, heads, blocks),
        out_shape=(
            jax.ShapeDtypeStruct((tokens, width), bf16),
            jax.ShapeDtypeStruct((tokens, width), bf16),
            jax.ShapeDtypeStruct((n, 2, tokens, head_dim), bf16),
        ),
        in_specs=[smem, smem, vmem, vmem, vmem],
        out_specs=(vmem, vmem, vmem),
        scratch_shapes=[
            pltpu.SMEM((n,), jnp.int32),
            pltpu.VMEM((blocks * rows, head_dim), bf16),
            pltpu.VMEM((blocks * rows, head_dim), bf16),
            pltpu.VMEM((2 * n // blocks, blocks * rows, wide), f32),
            pltpu.VMEM((head_dim, wide), f32),
            pltpu.VMEM((head_dim, wide), f32),
        ],
        compiler_params=pltpu.CompilerParams(vmem_limit_bytes=VMEM_LIMIT),
        name="attend",
    )(pair_order, doc_lengths, queries, grad_out, gathered)

    term = (2, tokens, head_dim)
    key_grad, value_grad = pl.pallas_call(
        functools.partial(scatter_kernel, n, head_dim ** (-0.5)),
        out_shape=(jax.ShapeDtypeStruct((tokens, head_dim), bf16),) * 2,
        in_specs=[vmem],
        out_specs=(vmem, vmem),
        scratch_shapes=[
            pltpu.VMEM((2, depth) + term, bf16),
            pltpu.VMEM((depth,) + term, bf16),
            pltpu.VMEM((depth,) + term, bf16),
            pltpu.VMEM((depth,) + term, bf16),
            pltpu.VMEM((depth,) + term, bf16),
            dma((2, depth)), dma((2, depth)), dma((depth, 2)), dma((depth, 2)),
            dma((depth, 2)), dma((depth, 2)),
        ],
        compiler_params=pltpu.CompilerParams(
            collective_id=1, has_side_effects=True, vmem_limit_bytes=VMEM_LIMIT
        ),
        name="scatter",
    )(terms)
    return attn_out, query_grad, key_grad, value_grad


def solution(mesh):
    tokens = P(("dp", "ctx"), None)
    return jax.shard_map(
        shards,
        mesh=mesh,
        in_specs=(tokens, tokens, tokens, tokens, P("dp"), P("dp")),
        out_specs=(tokens,) * 4,
        check_vma=False,
    )
```

```python
import functools

import jax
import jax.numpy as jnp
from jax import lax
from jax.experimental import pallas as pl
from jax.experimental.pallas import tpu as pltpu
from jax.sharding import PartitionSpec as P

MESH = pl.DeviceIdType.MESH
MIB = 1024 * 1024


def flip(index, mask):
    bit = 1
    while bit <= mask:
        if mask & bit:
            index = index + bit - 2 * bit * (lax.div(index, bit) % 2)
        bit *= 2
    return index


def place(n):
    me = lax.axis_index("ctx")
    core = me % 2
    x = lax.div(me, 2) % 2
    z = lax.div(me, 4)
    return z, x, core


def index_of(z, x, core):
    return (z * 2 + x) * 2 + core


def z_order(depth):
    return list(range(1, depth))


def greet(depth, z, x, core):
    barrier = pltpu.get_barrier_semaphore()
    peers = [index_of(flip(z, mask), x, core) for mask in z_order(depth)]
    peers += [index_of(z, 1 - x, core), index_of(z, x, 1 - core)]
    for peer in peers:
        pl.semaphore_signal(
            barrier, inc=1, device_id={"ctx": peer}, device_id_type=MESH
        )
    pl.semaphore_wait(barrier, len(peers))


def gather_kernel(n, k_ref, v_ref, all_ref, local_sem, zs, zr, xs, xr, cs, cr):
    depth = n // 4
    z, x, core = place(n)
    me = index_of(z, x, core)
    greet(depth, z, x, core)
    x_peer = index_of(z, 1 - x, core)
    c_peer = index_of(z, x, 1 - core)
    order = z_order(depth)
    sent = []

    def send(src, dst, send_sem, recv_sem, peer):
        copy = pltpu.make_async_remote_copy(
            src_ref=src, dst_ref=dst, send_sem=send_sem, recv_sem=recv_sem,
            device_id={"ctx": peer}, device_id_type=MESH,
        )
        copy.start()
        return copy

    def send_own(send_sem, recv_sem, peer):
        for part, ref in enumerate((k_ref, v_ref)):
            dst = all_ref.at[me, part]
            send(ref, dst, send_sem.at[part], recv_sem.at[part], peer)
            sent.append((dst, send_sem.at[part]))

    def wait_for(ref, sem):
        pltpu.make_async_copy(ref, ref, sem).wait()

    def pass_on(slot, arrived, routes):
        for part in range(2):
            ref = all_ref.at[slot, part]
            wait_for(ref, arrived.at[part])
            for send_sem, recv_sem, peer in routes:
                send(ref, ref, send_sem.at[part], recv_sem.at[part], peer)
                sent.append((ref, send_sem.at[part]))

    send_own(xs.at[0], xr.at[0], x_peer)
    for mask in order:
        send_own(zs.at[mask], zr.at[mask], index_of(flip(z, mask), x, core))
    send_own(cs.at[0, 0], cr.at[0, 0], c_peer)
    local = [
        pltpu.make_async_copy(ref, all_ref.at[me, part], local_sem.at[part])
        for part, ref in enumerate((k_ref, v_ref))
    ]
    for copy in local:
        copy.start()

    def from_z(mask):
        pass_on(
            index_of(flip(z, mask), x, core), zr.at[mask],
            [(xs.at[mask], xr.at[mask], x_peer), (cs.at[0, mask], cr.at[0, mask], c_peer)],
        )

    def from_x(mask):
        pass_on(
            index_of(flip(z, mask), 1 - x, core), xr.at[mask],
            [(cs.at[1, mask], cr.at[1, mask], c_peer)],
        )

    for mask in order:
        from_z(mask)
        if mask == 1:
            from_x(0)
    if depth == 1:
        from_x(0)
    for mask in order:
        from_x(mask)
    for mask in [0] + order:
        for side in range(2):
            slot = index_of(flip(z, mask), 1 - x if side else x, 1 - core)
            pass_on(slot, cr.at[side, mask], [])
    for copy in local:
        copy.wait()
    for ref, sem in sent:
        wait_for(ref, sem)


def scatter_kernel(
    n, scale, part_ref, kg_ref, vg_ref, r1, r2, r3, s1, s2, cs, cr, xs, xr, zs, zr
):
    depth = n // 4
    z, x, core = place(n)
    greet(depth, z, x, core)
    x_peer = index_of(z, 1 - x, core)
    c_peer = index_of(z, x, 1 - core)
    order = z_order(depth)[::-1] + [0]
    sent = []

    def send(src, dst, send_sem, recv_sem, peer):
        copy = pltpu.make_async_remote_copy(
            src_ref=src, dst_ref=dst, send_sem=send_sem, recv_sem=recv_sem,
            device_id={"ctx": peer}, device_id_type=MESH,
        )
        copy.start()
        sent.append(copy)
        return copy

    first, second, third = {}, {}, {}
    for side in (1, 0):
        for mask in order:
            row = flip(z, mask)
            slot = index_of(row, 1 - x if side else x, 1 - core)
            first[side, mask] = send(
                part_ref.at[slot], r1.at[side, mask],
                cs.at[side, mask], cr.at[side, mask], c_peer,
            )
    for mask in order:
        first[1, mask].wait_recv()
        for part in range(2):
            mine = part_ref[index_of(flip(z, mask), 1 - x, core), part].astype(jnp.float32)
            mine = mine + r1[1, mask, part].astype(jnp.float32)
            s1[mask, part] = mine.astype(jnp.bfloat16)
            second[mask, part] = send(
                s1.at[mask, part], r2.at[mask, part],
                xs.at[mask, part], xr.at[mask, part], x_peer,
            )
    total = [None, None]
    for mask in order:
        first[0, mask].wait_recv()
        for part in range(2):
            mine = part_ref[index_of(flip(z, mask), x, core), part].astype(jnp.float32)
            mine = mine + r1[0, mask, part].astype(jnp.float32)
            second[mask, part].wait_recv()
            mine = mine + r2[mask, part].astype(jnp.float32)
            if mask:
                s2[mask, part] = mine.astype(jnp.bfloat16)
                third[mask, part] = send(
                    s2.at[mask, part], r3.at[mask, part],
                    zs.at[mask, part], zr.at[mask, part],
                    index_of(flip(z, mask), x, core),
                )
            else:
                total[part] = mine
    for mask in order[:-1]:
        for part in range(2):
            third[mask, part].wait_recv()
            total[part] = total[part] + r3[mask, part].astype(jnp.float32)
    kg_ref[...] = (scale * total[0]).astype(kg_ref.dtype)
    vg_ref[...] = total[1].astype(vg_ref.dtype)
    for copy in sent:
        copy.wait_send()


def attend_kernel(
    n, heads, blocks, pair_ref, doc_ref, q_ref, g_ref, kv_ref,
    o_ref, dq_ref, part_ref, owner, k_buf, v_buf, e_buf, o_acc, dq_acc,
):
    tokens = q_ref.shape[0]
    rows = tokens // 2
    head_dim = q_ref.shape[1] // heads
    wide = heads * rows
    keys = blocks * rows
    scale = head_dim ** (-0.5)
    f32 = jnp.float32

    def put(i, carry):
        owner[pair_ref[i]] = i
        return carry

    lax.fori_loop(0, n, put, 0)
    part_ref[...] = jnp.zeros_like(part_ref)
    pair = pair_ref[lax.axis_index("ctx")]

    def locate(block):
        block = jnp.minimum(block, 2 * n - 1)
        late = block >= n
        dev = owner[jnp.where(late, 2 * n - 1 - block, block)]
        row = pl.multiple_of(jnp.where(late, rows, 0), rows)
        return dev, pl.ds(row, rows)

    def stack(ref, half):
        return jnp.concatenate(
            [
                ref[half * rows:(half + 1) * rows, h * head_dim:(h + 1) * head_dim]
                for h in range(heads)
            ],
            axis=0,
        )

    def unstack(ref, half, flat):
        for h in range(heads):
            ref[half * rows:(half + 1) * rows, h * head_dim:(h + 1) * head_dim] = flat[
                h * rows:(h + 1) * rows
            ].astype(ref.dtype)

    for half in range(2):
        block = 2 * n - 1 - pair if half else pair
        q_pos = block * rows + lax.broadcasted_iota(jnp.int32, (1, wide), 1) % rows

        def starts(i, carry):
            begin, of_rows, of_first = carry
            of_rows = jnp.where(begin <= q_pos, begin, of_rows)
            of_first = jnp.where(begin <= block * rows, begin, of_first)
            return begin + doc_ref[i], of_rows, of_first

        _, q_start, first = lax.fori_loop(
            0, doc_ref.shape[0], starts,
            (jnp.int32(0), jnp.zeros((1, wide), jnp.int32), jnp.int32(0)),
        )
        begin_block = lax.div(first, rows)
        chunks = lax.div(block - begin_block, blocks) + 1
        q_flat = stack(q_ref, half)
        g_flat = stack(g_ref, half)
        o_acc[...] = jnp.zeros_like(o_acc)
        dq_acc[...] = jnp.zeros_like(dq_acc)

        def fetch(chunk):
            for i in range(blocks):
                dev, where = locate(begin_block + chunk * blocks + i)
                k_buf[i * rows:(i + 1) * rows] = kv_ref[dev, 0, where, :]
                v_buf[i * rows:(i + 1) * rows] = kv_ref[dev, 1, where, :]
            return k_buf[...], v_buf[...]

        def forward(chunk, total):
            k, v = fetch(chunk)
            scores = lax.dot_general(
                k, q_flat, (((1,), (1,)), ((), ())), preferred_element_type=f32
            )
            k_pos = (begin_block + chunk * blocks) * rows + lax.broadcasted_iota(
                jnp.int32, (keys, 1), 0
            )
            seen = (k_pos >= q_start) & (k_pos <= q_pos)
            exp_scores = jnp.where(seen, jnp.exp(scores * scale), 0.0)
            e_buf[chunk] = exp_scores
            o_acc[...] += lax.dot_general(
                v, exp_scores.astype(jnp.bfloat16), (((0,), (0,)), ((), ())),
                preferred_element_type=f32,
            )
            return total + jnp.sum(exp_scores, axis=0, keepdims=True)

        total = lax.fori_loop(0, chunks, forward, jnp.zeros((1, wide), f32))
        inverse = 1.0 / total
        out = (o_acc[...] / total).astype(jnp.bfloat16).astype(f32)
        unstack(o_ref, half, out.T)
        row_dot = jnp.sum(g_flat.astype(f32).T * out, axis=0, keepdims=True)

        def backward(chunk, carry):
            k, v = fetch(chunk)
            prob = e_buf[chunk] * inverse
            grad_prob = lax.dot_general(
                v, g_flat, (((1,), (1,)), ((), ())), preferred_element_type=f32
            )
            grad_score = (prob * (grad_prob - row_dot)).astype(jnp.bfloat16)
            dq_acc[...] += lax.dot_general(
                k, grad_score, (((0,), (0,)), ((), ())), preferred_element_type=f32
            )
            dk = jnp.dot(grad_score, q_flat, preferred_element_type=f32)
            dv = jnp.dot(prob.astype(jnp.bfloat16), g_flat, preferred_element_type=f32)
            for i in range(blocks):
                at = begin_block + chunk * blocks + i
                dev, where = locate(at)

                @pl.when(at <= block)
                def _():
                    cut = slice(i * rows, (i + 1) * rows)
                    for side, grad in enumerate((dk, dv)):
                        old = part_ref[dev, side, where, :].astype(f32)
                        part_ref[dev, side, where, :] = (old + grad[cut]).astype(jnp.bfloat16)

            return carry

        lax.fori_loop(0, chunks, backward, 0)
        unstack(dq_ref, half, (scale * dq_acc[...]).T)


def shards(queries, keys, values, grad_out, pair_order, doc_lengths):
    tokens, width = queries.shape
    head_dim = keys.shape[1]
    heads = width // head_dim
    n = lax.axis_size("ctx")
    depth = n // 4
    blocks = 4
    vmem = pl.BlockSpec(memory_space=pltpu.VMEM)
    smem = pl.BlockSpec(memory_space=pltpu.SMEM)
    dma = pltpu.SemaphoreType.DMA
    bf16, f32 = jnp.bfloat16, jnp.float32

    gathered = pl.pallas_call(
        functools.partial(gather_kernel, n),
        out_shape=pltpu.VMEM((n, 2, tokens, head_dim), bf16),
        in_specs=[vmem] * 2,
        out_specs=vmem,
        scratch_shapes=[
            dma((2,)), dma((depth, 2)), dma((depth, 2)), dma((depth, 2)), dma((depth, 2)),
            dma((2, depth, 2)), dma((2, depth, 2)),
        ],
        compiler_params=pltpu.CompilerParams(
            collective_id=0, has_side_effects=True, vmem_limit_bytes=2 * MIB
        ),
        name="gather",
    )(keys, values)

    rows = tokens // 2
    wide = heads * rows
    chunks = pl.cdiv(n // 2 + 1, blocks)
    exp_bytes = 4 * chunks * blocks * rows * wide
    attn_out, query_grad, terms = pl.pallas_call(
        functools.partial(attend_kernel, n, heads, blocks),
        out_shape=(
            jax.ShapeDtypeStruct((tokens, width), bf16),
            jax.ShapeDtypeStruct((tokens, width), bf16),
            pltpu.VMEM((n, 2, tokens, head_dim), bf16),
        ),
        in_specs=[smem, smem, vmem, vmem, vmem],
        out_specs=(vmem, vmem, vmem),
        scratch_shapes=[
            pltpu.SMEM((n,), jnp.int32),
            pltpu.VMEM((blocks * rows, head_dim), bf16),
            pltpu.VMEM((blocks * rows, head_dim), bf16),
            pltpu.VMEM((chunks, blocks * rows, wide), f32),
            pltpu.VMEM((head_dim, wide), f32),
            pltpu.VMEM((head_dim, wide), f32),
        ],
        compiler_params=pltpu.CompilerParams(vmem_limit_bytes=exp_bytes + 10 * MIB),
        name="attend",
    )(pair_order, doc_lengths, queries, grad_out, gathered)

    term = (2, tokens, head_dim)
    key_grad, value_grad = pl.pallas_call(
        functools.partial(scatter_kernel, n, head_dim ** (-0.5)),
        out_shape=(pltpu.VMEM((tokens, head_dim), bf16),) * 2,
        in_specs=[vmem],
        out_specs=(vmem, vmem),
        scratch_shapes=[
            pltpu.VMEM((2, depth) + term, bf16),
            pltpu.VMEM((depth,) + term, bf16),
            pltpu.VMEM((depth,) + term, bf16),
            pltpu.VMEM((depth,) + term, bf16),
            pltpu.VMEM((depth,) + term, bf16),
            dma((2, depth)), dma((2, depth)), dma((depth, 2)), dma((depth, 2)),
            dma((depth, 2)), dma((depth, 2)),
        ],
        compiler_params=pltpu.CompilerParams(
            collective_id=1, has_side_effects=True,
            vmem_limit_bytes=6 * depth * 4 * tokens * head_dim + 2 * MIB,
        ),
        name="scatter",
    )(terms)
    return attn_out, query_grad, key_grad, value_grad


def solution(mesh):
    tokens = P(("dp", "ctx"), None)
    return jax.shard_map(
        shards,
        mesh=mesh,
        in_specs=(tokens, tokens, tokens, tokens, P("dp"), P("dp")),
        out_specs=(tokens,) * 4,
        check_vma=False,
    )
```

```python
import functools

import jax
import jax.numpy as jnp
from jax import lax
from jax.experimental import pallas as pl
from jax.experimental.pallas import tpu as pltpu
from jax.sharding import PartitionSpec as P

MESH = pl.DeviceIdType.MESH
MIB = 1024 * 1024


def flip(index, mask):
    bit = 1
    while bit <= mask:
        if mask & bit:
            index = index + bit - 2 * bit * (lax.div(index, bit) % 2)
        bit *= 2
    return index


def place(n):
    me = lax.axis_index("ctx")
    core = me % 2
    x = lax.div(me, 2) % 2
    z = lax.div(me, 4)
    return z, x, core


def index_of(z, x, core):
    return (z * 2 + x) * 2 + core


def z_order(depth):
    return list(range(1, depth))


def greet(depth, z, x, core):
    barrier = pltpu.get_barrier_semaphore()
    peers = [index_of(flip(z, mask), x, core) for mask in z_order(depth)]
    peers += [index_of(z, 1 - x, core), index_of(z, x, 1 - core)]
    for peer in peers:
        pl.semaphore_signal(
            barrier, inc=1, device_id={"ctx": peer}, device_id_type=MESH
        )
    pl.semaphore_wait(barrier, len(peers))


def gather_kernel(n, k_ref, v_ref, all_ref, local_sem, zs, zr, xs, xr, cs, cr):
    depth = n // 4
    z, x, core = place(n)
    me = index_of(z, x, core)
    local = [
        pltpu.make_async_copy(ref, all_ref.at[me, part], local_sem.at[part])
        for part, ref in enumerate((k_ref, v_ref))
    ]
    for copy in local:
        copy.start()
    greet(depth, z, x, core)
    for copy in local:
        copy.wait()
    x_peer = index_of(z, 1 - x, core)
    c_peer = index_of(z, x, 1 - core)
    order = z_order(depth)
    sent = []

    def send(src, dst, send_sem, recv_sem, peer):
        copy = pltpu.make_async_remote_copy(
            src_ref=src, dst_ref=dst, send_sem=send_sem, recv_sem=recv_sem,
            device_id={"ctx": peer}, device_id_type=MESH,
        )
        copy.start()
        return copy

    def send_own(send_sem, recv_sem, peer):
        for part in range(2):
            ref = all_ref.at[me, part]
            send(ref, ref, send_sem.at[part], recv_sem.at[part], peer)
            sent.append((ref, send_sem.at[part]))

    def wait_for(ref, sem):
        pltpu.make_async_copy(ref, ref, sem).wait()

    def pass_on(slot, arrived, routes):
        for part in range(2):
            ref = all_ref.at[slot, part]
            wait_for(ref, arrived.at[part])
            for send_sem, recv_sem, peer in routes:
                send(ref, ref, send_sem.at[part], recv_sem.at[part], peer)
                sent.append((ref, send_sem.at[part]))

    send_own(xs.at[0], xr.at[0], x_peer)
    for mask in order:
        send_own(zs.at[mask], zr.at[mask], index_of(flip(z, mask), x, core))
    send_own(cs.at[0, 0], cr.at[0, 0], c_peer)
    def from_z(mask):
        pass_on(
            index_of(flip(z, mask), x, core), zr.at[mask],
            [(xs.at[mask], xr.at[mask], x_peer), (cs.at[0, mask], cr.at[0, mask], c_peer)],
        )

    def from_x(mask):
        pass_on(
            index_of(flip(z, mask), 1 - x, core), xr.at[mask],
            [(cs.at[1, mask], cr.at[1, mask], c_peer)],
        )

    for mask in order:
        from_z(mask)
        if mask == 1:
            from_x(0)
    if depth == 1:
        from_x(0)
    for mask in order:
        from_x(mask)
    for mask in [0] + order:
        for side in range(2):
            slot = index_of(flip(z, mask), 1 - x if side else x, 1 - core)
            pass_on(slot, cr.at[side, mask], [])
    for ref, sem in sent:
        wait_for(ref, sem)


def scatter_kernel(
    n, scale, part_ref, kg_ref, vg_ref, r1, r2, r3, s1, s2, cs, cr, xs, xr, zs, zr
):
    depth = n // 4
    z, x, core = place(n)
    greet(depth, z, x, core)
    x_peer = index_of(z, 1 - x, core)
    c_peer = index_of(z, x, 1 - core)
    order = z_order(depth)[::-1] + [0]
    sent = []

    def send(src, dst, send_sem, recv_sem, peer):
        copy = pltpu.make_async_remote_copy(
            src_ref=src, dst_ref=dst, send_sem=send_sem, recv_sem=recv_sem,
            device_id={"ctx": peer}, device_id_type=MESH,
        )
        copy.start()
        sent.append(copy)
        return copy

    first, second, third = {}, {}, {}
    for side in (1, 0):
        for mask in order:
            row = flip(z, mask)
            slot = index_of(row, 1 - x if side else x, 1 - core)
            first[side, mask] = send(
                part_ref.at[slot], r1.at[side, mask],
                cs.at[side, mask], cr.at[side, mask], c_peer,
            )
    for mask in order:
        first[1, mask].wait_recv()
        for part in range(2):
            mine = part_ref[index_of(flip(z, mask), 1 - x, core), part].astype(jnp.float32)
            mine = mine + r1[1, mask, part].astype(jnp.float32)
            s1[mask, part] = mine.astype(jnp.bfloat16)
            second[mask, part] = send(
                s1.at[mask, part], r2.at[mask, part],
                xs.at[mask, part], xr.at[mask, part], x_peer,
            )
    total = [None, None]
    for mask in order:
        first[0, mask].wait_recv()
        for part in range(2):
            mine = part_ref[index_of(flip(z, mask), x, core), part].astype(jnp.float32)
            mine = mine + r1[0, mask, part].astype(jnp.float32)
            second[mask, part].wait_recv()
            mine = mine + r2[mask, part].astype(jnp.float32)
            if mask:
                s2[mask, part] = mine.astype(jnp.bfloat16)
                third[mask, part] = send(
                    s2.at[mask, part], r3.at[mask, part],
                    zs.at[mask, part], zr.at[mask, part],
                    index_of(flip(z, mask), x, core),
                )
            else:
                total[part] = mine
    for mask in order[:-1]:
        for part in range(2):
            third[mask, part].wait_recv()
            total[part] = total[part] + r3[mask, part].astype(jnp.float32)
    kg_ref[...] = (scale * total[0]).astype(kg_ref.dtype)
    vg_ref[...] = total[1].astype(vg_ref.dtype)
    for copy in sent:
        copy.wait_send()


def attend_kernel(
    n, heads, blocks, pair_ref, doc_ref, q_ref, g_ref, kv_ref,
    o_ref, dq_ref, part_ref, owner, k_buf, v_buf, e_buf, o_acc, dq_acc,
):
    tokens = q_ref.shape[0]
    rows = tokens // 2
    head_dim = q_ref.shape[1] // heads
    wide = heads * rows
    keys = blocks * rows
    scale = head_dim ** (-0.5)
    f32 = jnp.float32

    def put(i, carry):
        owner[pair_ref[i]] = i
        return carry

    lax.fori_loop(0, n, put, 0)
    part_ref[...] = jnp.zeros_like(part_ref)
    pair = pair_ref[lax.axis_index("ctx")]

    def locate(block):
        block = jnp.minimum(block, 2 * n - 1)
        late = block >= n
        dev = owner[jnp.where(late, 2 * n - 1 - block, block)]
        row = pl.multiple_of(jnp.where(late, rows, 0), rows)
        return dev, pl.ds(row, rows)

    def stack(ref, half):
        return jnp.concatenate(
            [
                ref[half * rows:(half + 1) * rows, h * head_dim:(h + 1) * head_dim]
                for h in range(heads)
            ],
            axis=0,
        )

    def unstack(ref, half, flat):
        for h in range(heads):
            ref[half * rows:(half + 1) * rows, h * head_dim:(h + 1) * head_dim] = flat[
                h * rows:(h + 1) * rows
            ].astype(ref.dtype)

    for half in range(2):
        block = 2 * n - 1 - pair if half else pair
        q_pos = block * rows + lax.broadcasted_iota(jnp.int32, (1, wide), 1) % rows

        def starts(i, carry):
            begin, of_rows, of_first = carry
            of_rows = jnp.where(begin <= q_pos, begin, of_rows)
            of_first = jnp.where(begin <= block * rows, begin, of_first)
            return begin + doc_ref[i], of_rows, of_first

        _, q_start, first = lax.fori_loop(
            0, doc_ref.shape[0], starts,
            (jnp.int32(0), jnp.zeros((1, wide), jnp.int32), jnp.int32(0)),
        )
        begin_block = lax.div(first, rows)
        chunks = lax.div(block - begin_block, blocks) + 1
        q_flat = stack(q_ref, half)
        g_flat = stack(g_ref, half)
        o_acc[...] = jnp.zeros_like(o_acc)
        dq_acc[...] = jnp.zeros_like(dq_acc)

        def fetch(chunk):
            for i in range(blocks):
                dev, where = locate(begin_block + chunk * blocks + i)
                k_buf[i * rows:(i + 1) * rows] = kv_ref[dev, 0, where, :]
                v_buf[i * rows:(i + 1) * rows] = kv_ref[dev, 1, where, :]
            return k_buf[...], v_buf[...]

        def forward(chunk, total):
            k, v = fetch(chunk)
            scores = lax.dot_general(
                k, q_flat, (((1,), (1,)), ((), ())), preferred_element_type=f32
            )
            k_pos = (begin_block + chunk * blocks) * rows + lax.broadcasted_iota(
                jnp.int32, (keys, 1), 0
            )
            seen = (k_pos >= q_start) & (k_pos <= q_pos)
            exp_scores = jnp.where(seen, jnp.exp(scores * scale), 0.0)
            e_buf[chunk] = exp_scores
            o_acc[...] += lax.dot_general(
                v, exp_scores.astype(jnp.bfloat16), (((0,), (0,)), ((), ())),
                preferred_element_type=f32,
            )
            return total + jnp.sum(exp_scores, axis=0, keepdims=True)

        total = lax.fori_loop(0, chunks, forward, jnp.zeros((1, wide), f32))
        inverse = 1.0 / total
        out = (o_acc[...] / total).astype(jnp.bfloat16).astype(f32)
        unstack(o_ref, half, out.T)
        row_dot = jnp.sum(g_flat.astype(f32).T * out, axis=0, keepdims=True)

        def backward(chunk, carry):
            k, v = fetch(chunk)
            prob = e_buf[chunk] * inverse
            grad_prob = lax.dot_general(
                v, g_flat, (((1,), (1,)), ((), ())), preferred_element_type=f32
            )
            grad_score = (prob * (grad_prob - row_dot)).astype(jnp.bfloat16)
            dq_acc[...] += lax.dot_general(
                k, grad_score, (((0,), (0,)), ((), ())), preferred_element_type=f32
            )
            dk = jnp.dot(grad_score, q_flat, preferred_element_type=f32)
            dv = jnp.dot(prob.astype(jnp.bfloat16), g_flat, preferred_element_type=f32)
            for i in range(blocks):
                at = begin_block + chunk * blocks + i
                dev, where = locate(at)

                @pl.when(at <= block)
                def _():
                    cut = slice(i * rows, (i + 1) * rows)
                    for side, grad in enumerate((dk, dv)):
                        old = part_ref[dev, side, where, :].astype(f32)
                        part_ref[dev, side, where, :] = (old + grad[cut]).astype(jnp.bfloat16)

            return carry

        lax.fori_loop(0, chunks, backward, 0)
        unstack(dq_ref, half, (scale * dq_acc[...]).T)


def shards(queries, keys, values, grad_out, pair_order, doc_lengths):
    tokens, width = queries.shape
    head_dim = keys.shape[1]
    heads = width // head_dim
    n = lax.axis_size("ctx")
    depth = n // 4
    blocks = 4
    vmem = pl.BlockSpec(memory_space=pltpu.VMEM)
    smem = pl.BlockSpec(memory_space=pltpu.SMEM)
    dma = pltpu.SemaphoreType.DMA
    bf16, f32 = jnp.bfloat16, jnp.float32

    gathered = pl.pallas_call(
        functools.partial(gather_kernel, n),
        out_shape=pltpu.VMEM((n, 2, tokens, head_dim), bf16),
        in_specs=[pl.BlockSpec(memory_space=pltpu.HBM)] * 2,
        out_specs=vmem,
        scratch_shapes=[
            dma((2,)), dma((depth, 2)), dma((depth, 2)), dma((depth, 2)), dma((depth, 2)),
            dma((2, depth, 2)), dma((2, depth, 2)),
        ],
        compiler_params=pltpu.CompilerParams(
            collective_id=0, has_side_effects=True, vmem_limit_bytes=2 * MIB
        ),
        name="gather",
    )(
        pltpu.with_memory_space_constraint(keys, pltpu.HBM),
        pltpu.with_memory_space_constraint(values, pltpu.HBM),
    )

    rows = tokens // 2
    wide = heads * rows
    chunks = pl.cdiv(n // 2 + 1, blocks)
    exp_bytes = 4 * chunks * blocks * rows * wide
    attn_out, query_grad, terms = pl.pallas_call(
        functools.partial(attend_kernel, n, heads, blocks),
        out_shape=(
            jax.ShapeDtypeStruct((tokens, width), bf16),
            jax.ShapeDtypeStruct((tokens, width), bf16),
            pltpu.VMEM((n, 2, tokens, head_dim), bf16),
        ),
        in_specs=[smem, smem, vmem, vmem, vmem],
        out_specs=(vmem, vmem, vmem),
        scratch_shapes=[
            pltpu.SMEM((n,), jnp.int32),
            pltpu.VMEM((blocks * rows, head_dim), bf16),
            pltpu.VMEM((blocks * rows, head_dim), bf16),
            pltpu.VMEM((chunks, blocks * rows, wide), f32),
            pltpu.VMEM((head_dim, wide), f32),
            pltpu.VMEM((head_dim, wide), f32),
        ],
        compiler_params=pltpu.CompilerParams(vmem_limit_bytes=exp_bytes + 10 * MIB),
        name="attend",
    )(pair_order, doc_lengths, queries, grad_out, gathered)

    term = (2, tokens, head_dim)
    key_grad, value_grad = pl.pallas_call(
        functools.partial(scatter_kernel, n, head_dim ** (-0.5)),
        out_shape=(pltpu.VMEM((tokens, head_dim), bf16),) * 2,
        in_specs=[vmem],
        out_specs=(vmem, vmem),
        scratch_shapes=[
            pltpu.VMEM((2, depth) + term, bf16),
            pltpu.VMEM((depth,) + term, bf16),
            pltpu.VMEM((depth,) + term, bf16),
            pltpu.VMEM((depth,) + term, bf16),
            pltpu.VMEM((depth,) + term, bf16),
            dma((2, depth)), dma((2, depth)), dma((depth, 2)), dma((depth, 2)),
            dma((depth, 2)), dma((depth, 2)),
        ],
        compiler_params=pltpu.CompilerParams(
            collective_id=1, has_side_effects=True,
            vmem_limit_bytes=6 * depth * 4 * tokens * head_dim + 2 * MIB,
        ),
        name="scatter",
    )(terms)
    return attn_out, query_grad, key_grad, value_grad


def solution(mesh):
    tokens = P(("dp", "ctx"), None)
    return jax.shard_map(
        shards,
        mesh=mesh,
        in_specs=(tokens, tokens, tokens, tokens, P("dp"), P("dp")),
        out_specs=(tokens,) * 4,
        check_vma=False,
    )
```
